32 devices in a mesh: tile: 8 (over z, x), pos: 4 (over y, core).
Axes of the slice: x: 2, y: 2, z: 4, core: 2. Of those that a mesh axis runs over, the one named last changes fastest.
Arguments:
- object_tiles: bfloat16 [8, 2, 512, 512], P('tile', None, 'pos'), may hold values from -4.1875 to 4.1875
- probe: float32 [2, 256, 256], replicated, may hold values from -4.2 to 4.2
- frames: bfloat16 [512, 256, 256], P(('tile', 'pos')), may hold values from 0 to 60, as said below
- offsets: int32 [2, 512], P(None, ('tile', 'pos')), may hold values from 1 to 511
Outputs:
- shifts: float32 [2, 512], P(None, ('tile', 'pos'))
- losses: float32 [512], P(('tile', 'pos'))
The draws below stay inside these ranges and needn't reach their ends.
Inputs may be any that keep to these rules, and one draw needn't show every extreme that they name: `frames`: amplitudes are not negative.
All inputs are finite; a program needn't handle non-finite values.
Results may differ from the reference program's by a relative error of at most 0.0097.
Values may be sent and summed in bfloat16 or wider, within the bound.
A program may use at most 128 MiB of HBM per device.

```python
import math
import jax
import jax.numpy as jnp
from jax import lax

PROBE = 256
GC = 4
POS_DEV = 16
CORE = 512
TILES = 8
POSITIONS = 512
N_TILE = 8
N_POS = 4


def draw_frames(key, part):
    ramp_scale = 1.0 + 2.0 * jnp.arange(POSITIONS, dtype=jnp.float32) / (POSITIONS - 1)
    normal_base = jax.random.normal(jax.random.fold_in(key, 5), (POSITIONS, PROBE, PROBE), jnp.float32)
    amplitude = jnp.minimum(jnp.abs(normal_base), 5.0) * ramp_scale[:, None, None]
    return amplitude.astype(jnp.bfloat16)


def with_ends(values, key, low, high):
    extent = values.shape
    index_at = [jax.random.randint(jax.random.fold_in(key, axis), (), 0, extent[axis]) for axis in range(len(extent))]
    values = values.at[tuple(index_at)].set(low)
    longest = extent.index(max(extent))
    index_at[longest] = (index_at[longest] + 1) % extent[longest]
    return values.at[tuple(index_at)].set(high)


def levels(stream_key, extent, split, least, high):
    loudness, own = 1.0, jax.random.fold_in(stream_key, 6)
    for dim, blocks in split:
        heights = jnp.exp(jax.random.uniform(jax.random.fold_in(own, dim), (blocks,), jnp.float32, least / len(split), high / len(split)))
        loudness = loudness * jnp.repeat(heights, extent[dim] // blocks).reshape([-1 if axis == dim else 1 for axis in range(len(extent))])
    return loudness


def centred(stream_key, dims, deviation, limit, split=(), kind=jnp.bfloat16):
    result = deviation * jax.random.normal(stream_key, dims, jnp.float32)
    if split:
        result = result * levels(stream_key, dims, split, -0.22, 0.18)
    return jnp.clip(result, -limit, limit).astype(kind)


def setup_inputs(seed: int = 0) -> dict:
    key_of = jax.random.split(jax.random.key(seed), 5)
    object_tiles = centred(key_of[0], (TILES, 2, CORE, CORE), 0.7, 4.1875, ((0, 8), (2, 4)))
    probe = centred(key_of[1], (2, PROBE, PROBE), 0.7, 4.2, (), jnp.float32)
    frames = draw_frames(jax.random.fold_in(key_of[4], 71), 0)
    offsets = with_ends(jax.random.randint(key_of[3], (2, POSITIONS), 1, CORE), jax.random.fold_in(key_of[3], 1), 1, CORE - 1).astype(jnp.int32)
    return dict(object_tiles=object_tiles, probe=probe, frames=frames, offsets=offsets)


def dft_tables(length_n):
    indices = jnp.arange(length_n, dtype=jnp.int32)
    products_mod = indices[:, None] * indices[None, :] % length_n
    angles = products_mod.astype(jnp.float32) * (2.0 * math.pi / length_n)
    factor = 1.0 / math.sqrt(length_n)
    return ((jnp.cos(angles) * factor).astype(jnp.bfloat16), (jnp.sin(angles) * factor).astype(jnp.bfloat16))

def matmul(left_m, right_m):
    return jnp.dot(left_m, right_m, preferred_element_type=jnp.float32)

def refine_ref(window, probe, detector, cosine_table, sine_table):
    window_f = window.astype(jnp.float32)
    patch = window_f[:, 1:-1, 1:-1]
    along_row = 0.5 * (window_f[:, 2:, 1:-1] - window_f[:, :-2, 1:-1])
    along_col = 0.5 * (window_f[:, 1:-1, 2:] - window_f[:, 1:-1, :-2])
    exit_re = (probe[0] * patch[0] - probe[1] * patch[1]).astype(jnp.bfloat16)
    exit_im = (probe[0] * patch[1] + probe[1] * patch[0]).astype(jnp.bfloat16)
    half_re = (matmul(cosine_table, exit_re) + matmul(sine_table, exit_im)).astype(jnp.bfloat16)
    half_im = (matmul(cosine_table, exit_im) - matmul(sine_table, exit_re)).astype(jnp.bfloat16)
    far_re = matmul(half_re, cosine_table) + matmul(half_im, sine_table)
    far_im = matmul(half_im, cosine_table) - matmul(half_re, sine_table)
    magnitude = jnp.sqrt(far_re * far_re + far_im * far_im)
    keep_part = 1.0 - detector.astype(jnp.float32) / jnp.maximum(magnitude, 0.25)
    resid_re = far_re * keep_part
    resid_im = far_im * keep_part
    loss_one = jnp.mean(resid_re * resid_re + resid_im * resid_im)
    round_re = resid_re.astype(jnp.bfloat16)
    round_im = resid_im.astype(jnp.bfloat16)
    inner_re = (matmul(cosine_table, round_re) - matmul(sine_table, round_im)).astype(jnp.bfloat16)
    inner_im = (matmul(cosine_table, round_im) + matmul(sine_table, round_re)).astype(jnp.bfloat16)
    wave_re = matmul(inner_re, cosine_table) - matmul(inner_im, sine_table)
    wave_im = matmul(inner_im, cosine_table) + matmul(inner_re, sine_table)

    def slope_of(derived):
        probed_re = probe[0] * derived[0] - probe[1] * derived[1]
        probed_im = probe[0] * derived[1] + probe[1] * derived[0]
        return jnp.sum(wave_re * probed_re + wave_im * probed_im)
    return (jnp.stack([slope_of(along_row), slope_of(along_col)]), loss_one)

def reference(object_tiles, probe, frames, offsets):
    region_rows = N_TILE // GC
    region_grid = object_tiles.reshape(region_rows, GC, 2, CORE, CORE)
    full_object = region_grid.transpose(2, 0, 3, 1, 4).reshape(2, region_rows * CORE, GC * CORE)
    margin = PROBE // 2
    padded = jnp.pad(full_object, ((0, 0), (margin, margin), (margin, margin)))
    indices = jnp.arange(POSITIONS, dtype=jnp.int32)
    region_of = indices // (POS_DEV * N_POS)
    starts_row = region_of // GC * CORE + offsets[0] - 1
    starts_col = region_of % GC * CORE + offsets[1] - 1
    cosine_table, sine_table = dft_tables(PROBE)

    def refine_at(position):
        detector, start_row, start_col = position
        window = lax.dynamic_slice(padded, (jnp.zeros((), jnp.int32), start_row.astype(jnp.int32), start_col.astype(jnp.int32)), (2, PROBE + 2, PROBE + 2))
        return refine_ref(window, probe, detector, cosine_table, sine_table)
    slopes, losses = lax.map(refine_at, (frames, starts_row, starts_col))
    total_sq = jnp.sum(slopes * slopes)
    norm_scale = jnp.sqrt(total_sq / POSITIONS + 1e-06)
    return ((-slopes / norm_scale).T, losses)
```

```python
import functools
import math

import jax
import jax.numpy as jnp
import numpy as np
from jax import lax
from jax.experimental import pallas as pl
from jax.experimental.pallas import tpu as pltpu
from jax.sharding import PartitionSpec as P

GC = 4
CHUNKS = 4
BATCH = 2
MESH_ID = pl.DeviceIdType.MESH


def dft_tables(length_n):
    indices = np.arange(length_n)
    products_mod = indices[:, None] * indices[None, :] % length_n
    angles = products_mod.astype(np.float32) * np.float32(2.0 * math.pi / length_n)
    factor = np.float32(1.0 / math.sqrt(length_n))
    cosine, sine = np.cos(angles) * factor, np.sin(angles) * factor
    forward = np.block([[cosine, sine], [-sine, cosine]])
    return jnp.asarray(forward, jnp.bfloat16), jnp.asarray(forward.T, jnp.bfloat16)


def halo_kernel(n_tile, margin, x_ref, pad_ref, send_sems, recv_sems, local_sem):
    t, p = lax.axis_index("tile"), lax.axis_index("pos")
    _, quarter, width = x_ref.shape
    rows = pad_ref.shape[1] - 2 * margin
    last = rows // quarter - 1
    c, r = t % GC, t // GC
    core, half = p % 2, p // 2
    near, far = p + 1 - 2 * core, p + 2 - 4 * half
    west, east = c > 0, c < GC - 1
    north, south = r > 0, r < n_tile // GC - 1
    yes = p >= 0
    is_first, is_last = p == 0, p == last
    tall, wide = rows + 2 * margin, width + 2 * margin

    def zero(cond, rows_at, cols_at):
        @pl.when(cond)
        def _():
            part = pad_ref.at[:, rows_at, cols_at]
            part[...] = jnp.zeros(part.shape, part.dtype)

    zero(jnp.logical_not(west), slice(0, tall), slice(0, margin))
    zero(jnp.logical_not(east), slice(0, tall), slice(margin + width, wide))
    zero(jnp.logical_not(north), slice(0, margin), slice(0, wide))
    zero(jnp.logical_not(south), slice(margin + rows, tall), slice(0, wide))

    barrier = pltpu.get_barrier_semaphore()
    is_end = jnp.logical_or(is_first, is_last)
    partners = [
        (yes, t, near),
        (yes, t, far),
        (west, t - 1, p),
        (east, t + 1, p),
        (jnp.logical_and(is_end, north), t - GC, p),
        (jnp.logical_and(is_end, south), t + GC, p),
    ]
    for cond, to_t, to_p in partners:
        @pl.when(cond)
        def _():
            pl.semaphore_signal(barrier, inc=1, device_id=(to_t, to_p), device_id_type=MESH_ID)
    ends = is_end.astype(jnp.int32)
    sides_met = west.astype(jnp.int32) + east.astype(jnp.int32)
    rows_met = north.astype(jnp.int32) + south.astype(jnp.int32)
    pl.semaphore_wait(barrier, 2 + sides_met + ends * rows_met)

    mine = pl.ds(pl.multiple_of(margin + p * quarter, quarter), quarter)
    its = pl.ds(pl.multiple_of(margin + far * quarter, quarter), quarter)
    nears = pl.ds(pl.multiple_of(margin + near * quarter, quarter), quarter)
    near_far = near + 2 - 4 * half
    nears_far = pl.ds(pl.multiple_of(margin + near_far * quarter, quarter), quarter)
    mid = slice(margin, margin + width)
    left, right = slice(0, margin), slice(margin + width, wide)
    every = slice(0, wide)
    sent = []

    def copy(index, src, dst, to_t, to_p):
        return pltpu.make_async_remote_copy(
            src_ref=src,
            dst_ref=dst,
            send_sem=send_sems.at[index],
            recv_sem=recv_sems.at[index],
            device_id=(to_t, to_p),
            device_id_type=MESH_ID,
        )

    def send(cond, index, src, dst, to_t, to_p):
        made = copy(index, src, dst, to_t, to_p)
        sent.append((cond, made))

        @pl.when(cond)
        def _():
            made.start()

    def receive(cond, index, dst):
        @pl.when(cond)
        def _():
            copy(index, dst, dst, t, near).wait_recv()

    def at(rows_at, cols_at):
        return pad_ref.at[:, rows_at, cols_at]

    own = pltpu.make_async_copy(x_ref, at(mine, mid), local_sem)
    own.start()
    send(east, 2, x_ref.at[:, :, width - margin : width], at(mine, left), t + 1, p)
    send(west, 3, x_ref.at[:, :, 0:margin], at(mine, right), t - 1, p)
    send(yes, 0, x_ref, at(mine, mid), t, far)
    send(yes, 1, x_ref, at(mine, mid), t, near)
    own.wait()
    receive(west, 2, at(mine, left))
    receive(east, 3, at(mine, right))
    piece = margin // CHUNKS
    base = 11
    for k in range(CHUNKS):
        up, down = slice(margin + rows + k * piece, margin + rows + (k + 1) * piece), slice(k * piece, (k + 1) * piece)
        top = slice(margin + k * piece, margin + (k + 1) * piece)
        bottom = slice(rows + k * piece, rows + (k + 1) * piece)
        send(jnp.logical_and(is_first, north), base + k, at(top, every), at(up, every), t - GC, p)
        send(jnp.logical_and(is_last, south), base + 3 * CHUNKS + k, at(bottom, every), at(down, every), t + GC, p)
    send(yes, 4, at(mine, left), at(mine, left), t, far)
    send(yes, 5, at(mine, right), at(mine, right), t, far)
    send(yes, 7, at(mine, left), at(mine, left), t, near)
    send(yes, 8, at(mine, right), at(mine, right), t, near)
    receive(yes, 0, at(its, mid))
    send(yes, 6, at(its, mid), at(its, mid), t, near)
    receive(yes, 4, at(its, left))
    send(yes, 9, at(its, left), at(its, left), t, near)
    receive(yes, 5, at(its, right))
    send(yes, 10, at(its, right), at(its, right), t, near)
    sides = [
        (base, south, margin + rows, is_first, core == 0),
        (base + 3 * CHUNKS, north, 0, is_last, core == 1),
    ]
    for start, inside, row, is_root, is_side in sides:
        for k in range(CHUNKS):
            part = at(slice(row + k * piece, row + (k + 1) * piece), every)
            root = jnp.logical_and(inside, is_root)
            holds = jnp.logical_and(inside, is_side)
            second = jnp.logical_and(holds, jnp.logical_not(is_root))
            receive(root, start + k, part)
            send(root, start + CHUNKS + k, part, part, t, far)
            receive(second, start + CHUNKS + k, part)
            send(holds, start + 2 * CHUNKS + k, part, part, t, near)
    receive(yes, 1, at(nears, mid))
    receive(yes, 7, at(nears, left))
    receive(yes, 8, at(nears, right))
    receive(yes, 6, at(nears_far, mid))
    receive(yes, 9, at(nears_far, left))
    receive(yes, 10, at(nears_far, right))
    for start, inside, row, is_root, is_side in sides:
        for k in range(CHUNKS):
            part = at(slice(row + k * piece, row + (k + 1) * piece), every)
            receive(jnp.logical_and(inside, jnp.logical_not(is_side)), start + 2 * CHUNKS + k, part)
    for cond, made in sent:
        @pl.when(cond)
        def _():
            made.wait_send()


def gather_halo(quarter, n_tile, n_pos, margin):
    if n_pos != 4 or quarter.shape[1] < margin:
        raise ValueError("unsupported split")
    rows = quarter.shape[1] * n_pos
    sems = 11 + 6 * CHUNKS
    return pl.pallas_call(
        functools.partial(halo_kernel, n_tile, margin),
        out_shape=jax.ShapeDtypeStruct((2, rows + 2 * margin, quarter.shape[2] + 2 * margin), quarter.dtype),
        in_specs=[pl.BlockSpec(memory_space=pltpu.VMEM)],
        out_specs=pl.BlockSpec(memory_space=pltpu.VMEM),
        scratch_shapes=[
            pltpu.SemaphoreType.DMA((sems,)),
            pltpu.SemaphoreType.DMA((sems,)),
            pltpu.SemaphoreType.DMA,
        ],
        compiler_params=pltpu.CompilerParams(collective_id=0, has_side_effects=True),
    )(quarter)


def fold(value):
    return jnp.sum(value.reshape(-1, 8, value.shape[-1]), axis=0)


def refine_kernel(
    batch, steps, off_ref, pad_ref, probe_ref, frames_ref, fwd_ref, bwd_ref, out_ref,
    planes, patch, slant, exits, halves, resid, inner, sums,
):
    step = pl.program_id(0)
    n = probe_ref.shape[1]
    tall, wide = pad_ref.shape[1], pad_ref.shape[2]
    lanes = 128
    blocks = n // lanes

    @pl.when(step == 0)
    def _():
        @pl.loop(0, tall // 32)
        def _(i):
            at = pl.ds(pl.multiple_of(i * 32, 32), 32)
            for part in range(2):
                value = pad_ref[part, at, :].astype(jnp.float32)
                slope = 0.5 * (pltpu.roll(value, wide - 1, 1) - pltpu.roll(value, 1, 1))
                for k in range(wide // lanes):
                    cols = slice(k * lanes, (k + 1) * lanes)
                    planes[part, k, at, :] = value[:, cols]
                    planes[2 + part, k, at, :] = slope[:, cols]

    column = lax.broadcasted_iota(jnp.int32, (8, lanes), 1)

    for b in range(batch):
        j = step * batch + b
        row, col = off_ref[0, j], off_ref[1, j]
        block, shift = col // lanes, col % lanes
        turn = (lanes - shift) % lanes
        for part in range(4):
            high = n + 8 if part < 2 else n
            first = row - 1 if part < 2 else row
            target = patch.at[b, part] if part < 2 else slant.at[b, part - 2]
            keep = lax.broadcasted_iota(jnp.int32, (high, lanes), 1) < lanes - shift
            turned = [
                pltpu.roll(planes[part, block + k, pl.ds(first, high), :], turn, 1) for k in range(blocks + 1)
            ]
            for k in range(blocks):
                target[:, k * lanes : (k + 1) * lanes] = jnp.where(keep, turned[k], turned[k + 1])
        o_re, o_im = patch[b, 0, 1 : n + 1, :], patch[b, 1, 1 : n + 1, :]
        p_re, p_im = probe_ref[0], probe_ref[1]
        exits[b, :n, :] = (p_re * o_re - p_im * o_im).astype(jnp.bfloat16)
        exits[b, n:, :] = (p_re * o_im + p_im * o_re).astype(jnp.bfloat16)
    for b in range(batch):
        half = jnp.dot(fwd_ref[...], exits[b], preferred_element_type=jnp.float32)
        halves[b * n : (b + 1) * n, :n] = half[:n].astype(jnp.bfloat16)
        halves[b * n : (b + 1) * n, n:] = half[n:].astype(jnp.bfloat16)
    losses = []
    for b in range(batch):
        wave = jnp.dot(halves[b * n : (b + 1) * n, :], bwd_ref[...], preferred_element_type=jnp.float32)
        f_re, f_im = wave[:, :n], wave[:, n:]
        square = f_re * f_re + f_im * f_im
        keep_part = 1.0 - frames_ref[b].astype(jnp.float32) * lax.rsqrt(jnp.maximum(square, 0.0625))
        losses.append(fold(square * (keep_part * keep_part)))
        resid[b, :n, :] = (f_re * keep_part).astype(jnp.bfloat16)
        resid[b, n:, :] = (f_im * keep_part).astype(jnp.bfloat16)
    for b in range(batch):
        back = jnp.dot(bwd_ref[...], resid[b], preferred_element_type=jnp.float32)
        inner[b * n : (b + 1) * n, :n] = back[:n].astype(jnp.bfloat16)
        inner[b * n : (b + 1) * n, n:] = back[n:].astype(jnp.bfloat16)
    for b in range(batch):
        j = step * batch + b
        wave = jnp.dot(inner[b * n : (b + 1) * n, :], fwd_ref[...], preferred_element_type=jnp.float32)
        g_re, g_im = wave[:, :n], wave[:, n:]
        p_re, p_im = probe_ref[0], probe_ref[1]
        q_re = g_re * p_re + g_im * p_im
        q_im = g_re * p_im - g_im * p_re
        d_re = patch[b, 0, 2 : n + 2, :] - patch[b, 0, 0:n, :]
        d_im = patch[b, 1, 2 : n + 2, :] - patch[b, 1, 0:n, :]
        by_row = fold(q_re * d_re - q_im * d_im) * 0.5
        by_col = fold(q_re * slant[b, 0] - q_im * slant[b, 1])
        for which, value in enumerate((by_row, by_col, losses[b] * (1.0 / (n * n)))):
            line = jnp.sum(value, axis=0, keepdims=True)
            short = line[:, :lanes]
            for k in range(1, blocks):
                short = short + line[:, k * lanes : (k + 1) * lanes]
            sums[which, pl.ds(j, 1), :] = short

    @pl.when(step == steps - 1)
    def _():
        count = sums.shape[1]
        diagonal = lax.broadcasted_iota(jnp.int32, (count, lanes), 0) == lax.broadcasted_iota(jnp.int32, (count, lanes), 1)
        lines = []
        for which in range(3):
            full = jnp.sum(sums[which], axis=1, keepdims=True)
            lines.append(jnp.sum(jnp.where(diagonal, full, 0.0), axis=0, keepdims=True))
        squares = jnp.sum(lines[0] * lines[0] + lines[1] * lines[1], axis=1, keepdims=True)
        lines.append(jnp.broadcast_to(squares, (1, lanes)))
        out_ref[...] = jnp.concatenate(lines + [jnp.zeros((4, lanes), jnp.float32)], axis=0)


def refine(padded, probe, frames, offsets):
    count, n, _ = frames.shape
    if count % BATCH or count > 128 or n % 128:
        raise ValueError("unsupported sizes")
    forward, backward = dft_tables(n)
    tall, wide = padded.shape[1:]
    steps = count // BATCH
    vmem = lambda shape, kind: pltpu.VMEM(shape, kind)
    whole = lambda shape: pl.BlockSpec(shape, lambda i: (0,) * len(shape))
    return pl.pallas_call(
        functools.partial(refine_kernel, BATCH, steps),
        grid=(steps,),
        out_shape=jax.ShapeDtypeStruct((8, 128), jnp.float32),
        in_specs=[
            pl.BlockSpec(memory_space=pltpu.SMEM),
            whole(padded.shape),
            whole(probe.shape),
            pl.BlockSpec((BATCH, n, n), lambda i: (i, 0, 0)),
            whole(forward.shape),
            whole(backward.shape),
        ],
        out_specs=whole((8, 128)),
        scratch_shapes=[
            vmem((4, wide // 128, tall + 8, 128), jnp.float32),
            vmem((BATCH, 2, n + 8, n), jnp.float32),
            vmem((BATCH, 2, n, n), jnp.float32),
            vmem((BATCH, 2 * n, n), jnp.bfloat16),
            vmem((BATCH * n, 2 * n), jnp.bfloat16),
            vmem((BATCH, 2 * n, n), jnp.bfloat16),
            vmem((BATCH * n, 2 * n), jnp.bfloat16),
            vmem((3, count, 128), jnp.float32),
        ],
        compiler_params=pltpu.CompilerParams(vmem_limit_bytes=56 * 1024 * 1024),
    )(offsets, padded, probe, frames, forward, backward)


def scale_kernel(n_tile, n_pos, positions, mine_ref, shifts_ref, losses_ref, others, send_sems, recv_sems):
    devices = n_tile * n_pos
    me = lax.axis_index("tile") * n_pos + lax.axis_index("pos")
    count = shifts_ref.shape[1]

    def to(k):
        other = (me + k) % devices
        return (other // n_pos, other % n_pos)

    barrier = pltpu.get_barrier_semaphore()

    def greet(k, carry):
        pl.semaphore_signal(barrier, inc=1, device_id=to(k), device_id_type=MESH_ID)
        return carry

    lax.fori_loop(1, devices, greet, 0)
    pl.semaphore_wait(barrier, devices - 1)

    def copy(k):
        return pltpu.make_async_remote_copy(
            src_ref=mine_ref,
            dst_ref=others.at[k - 1],
            send_sem=send_sems.at[k - 1],
            recv_sem=recv_sems.at[k - 1],
            device_id=to(k),
            device_id_type=MESH_ID,
        )

    def begin(k, carry):
        copy(k).start()
        return carry

    def finish(k, carry):
        copy(k).wait()
        return carry

    lax.fori_loop(1, devices, begin, 0)
    lax.fori_loop(1, devices, finish, 0)
    total = jnp.sum(others[...], axis=0) + mine_ref[...]
    scale = jnp.sqrt(total[3:4, :] * (1.0 / positions) + 1e-06)
    shifts_ref[...] = (-mine_ref[0:2, :] / scale)[:, :count]
    losses_ref[...] = mine_ref[2:3, :count]


def normalise(lines, count, n_tile, n_pos):
    devices = n_tile * n_pos
    whole = pl.BlockSpec(memory_space=pltpu.VMEM)
    return pl.pallas_call(
        functools.partial(scale_kernel, n_tile, n_pos, count * devices),
        out_shape=(jax.ShapeDtypeStruct((2, count), jnp.float32), jax.ShapeDtypeStruct((1, count), jnp.float32)),
        in_specs=[whole],
        out_specs=(whole, whole),
        scratch_shapes=[
            pltpu.VMEM((devices - 1, 8, 128), jnp.float32),
            pltpu.SemaphoreType.DMA((devices - 1,)),
            pltpu.SemaphoreType.DMA((devices - 1,)),
        ],
        compiler_params=pltpu.CompilerParams(collective_id=1, has_side_effects=True),
    )(lines)


def solution(mesh):
    n_tile, n_pos = mesh.shape["tile"], mesh.shape["pos"]

    def local(object_tiles, probe, frames, offsets):
        padded = gather_halo(object_tiles[0], n_tile, n_pos, probe.shape[1] // 2)
        lines = refine(padded, probe, frames, offsets)
        shifts, losses = normalise(lines, frames.shape[0], n_tile, n_pos)
        return shifts, losses[0]

    in_specs = (
        P("tile", None, "pos", None),
        P(),
        P(("tile", "pos"), None, None),
        P(None, ("tile", "pos")),
    )
    out_specs = (P(None, ("tile", "pos")), P(("tile", "pos")))
    return jax.shard_map(local, mesh=mesh, in_specs=in_specs, out_specs=out_specs, check_vma=False)
```

```python
import functools
import math

import jax
import jax.numpy as jnp
import numpy as np
from jax import lax
from jax.experimental import pallas as pl
from jax.experimental.pallas import tpu as pltpu
from jax.sharding import PartitionSpec as P

GC = 4
CHUNKS = 4
BATCH = 2
MESH_ID = pl.DeviceIdType.MESH


def dft_tables(length_n):
    indices = np.arange(length_n)
    products_mod = indices[:, None] * indices[None, :] % length_n
    angles = products_mod.astype(np.float32) * np.float32(2.0 * math.pi / length_n)
    factor = np.float32(1.0 / math.sqrt(length_n))
    cosine, sine = np.cos(angles) * factor, np.sin(angles) * factor
    forward = np.block([[cosine, sine], [-sine, cosine]])
    return jnp.asarray(forward, jnp.bfloat16), jnp.asarray(forward.T, jnp.bfloat16)


def peer(axis, k, n_tile, n_pos):
    t, p = lax.axis_index("tile"), lax.axis_index("pos")
    if axis == "pos":
        return (t, lax.rem(p + k, n_pos))
    return (lax.rem(t + k, n_tile), p)


def gather_halo(n_tile, n_pos, margin, x_ref, pad_ref, send_sems, recv_sems, local_sem, convert):
    t, p = lax.axis_index("tile"), lax.axis_index("pos")
    _, quarter, width = x_ref.shape
    rows = pad_ref.shape[1] - 2 * margin
    last = rows // quarter - 1
    c, r = t % GC, t // GC
    core, half = p % 2, p // 2
    near, far = p + 1 - 2 * core, p + 2 - 4 * half
    west, east = c > 0, c < GC - 1
    north, south = r > 0, r < n_tile // GC - 1
    yes = p >= 0
    is_first, is_last = p == 0, p == last
    tall, wide = rows + 2 * margin, width + 2 * margin

    def zero(cond, rows_at, cols_at):
        @pl.when(cond)
        def _():
            part = pad_ref.at[:, rows_at, cols_at]
            part[...] = jnp.zeros(part.shape, part.dtype)

    zero(jnp.logical_not(west), slice(0, tall), slice(0, margin))
    zero(jnp.logical_not(east), slice(0, tall), slice(margin + width, wide))
    zero(jnp.logical_not(north), slice(0, margin), slice(0, wide))
    zero(jnp.logical_not(south), slice(margin + rows, tall), slice(0, wide))

    barrier = pltpu.get_barrier_semaphore()
    for axis, devices in (("pos", n_pos), ("tile", n_tile)):
        for k in range(1, devices):
            pl.semaphore_signal(barrier, inc=1, device_id=peer(axis, k, n_tile, n_pos), device_id_type=MESH_ID)
    pl.semaphore_wait(barrier, n_pos + n_tile - 2)

    mine = pl.ds(pl.multiple_of(margin + p * quarter, quarter), quarter)
    its = pl.ds(pl.multiple_of(margin + far * quarter, quarter), quarter)
    nears = pl.ds(pl.multiple_of(margin + near * quarter, quarter), quarter)
    near_far = near + 2 - 4 * half
    nears_far = pl.ds(pl.multiple_of(margin + near_far * quarter, quarter), quarter)
    mid = slice(margin, margin + width)
    left, right = slice(0, margin), slice(margin + width, wide)
    every = slice(0, wide)
    sent = []

    def copy(index, src, dst, to_t, to_p):
        return pltpu.make_async_remote_copy(
            src_ref=src,
            dst_ref=dst,
            send_sem=send_sems.at[index],
            recv_sem=recv_sems.at[index],
            device_id=(to_t, to_p),
            device_id_type=MESH_ID,
        )

    def send(cond, index, src, dst, to_t, to_p):
        made = copy(index, src, dst, to_t, to_p)
        sent.append((cond, made))

        @pl.when(cond)
        def _():
            made.start()

    def receive(cond, index, dst):
        @pl.when(cond)
        def _():
            copy(index, dst, dst, t, near).wait_recv()

    def at(rows_at, cols_at):
        return pad_ref.at[:, rows_at, cols_at]

    own = pltpu.make_async_copy(x_ref, at(mine, mid), local_sem)
    own.start()
    send(east, 2, x_ref.at[:, :, width - margin : width], at(mine, left), t + 1, p)
    send(west, 3, x_ref.at[:, :, 0:margin], at(mine, right), t - 1, p)
    send(yes, 0, x_ref, at(mine, mid), t, far)
    send(yes, 1, x_ref, at(mine, mid), t, near)
    own.wait()
    receive(west, 2, at(mine, left))
    receive(east, 3, at(mine, right))
    piece = margin // CHUNKS
    base = 11
    for k in range(CHUNKS):
        up, down = slice(margin + rows + k * piece, margin + rows + (k + 1) * piece), slice(k * piece, (k + 1) * piece)
        top = slice(margin + k * piece, margin + (k + 1) * piece)
        bottom = slice(rows + k * piece, rows + (k + 1) * piece)
        send(jnp.logical_and(is_first, north), base + k, at(top, every), at(up, every), t - GC, p)
        send(jnp.logical_and(is_last, south), base + 3 * CHUNKS + k, at(bottom, every), at(down, every), t + GC, p)
    send(yes, 4, at(mine, left), at(mine, left), t, far)
    send(yes, 5, at(mine, right), at(mine, right), t, far)
    send(yes, 7, at(mine, left), at(mine, left), t, near)
    send(yes, 8, at(mine, right), at(mine, right), t, near)
    receive(yes, 0, at(its, mid))
    send(yes, 6, at(its, mid), at(its, mid), t, near)
    receive(yes, 4, at(its, left))
    send(yes, 9, at(its, left), at(its, left), t, near)
    receive(yes, 5, at(its, right))
    send(yes, 10, at(its, right), at(its, right), t, near)
    sides = [
        (base, south, margin + rows, is_first, core == 0),
        (base + 3 * CHUNKS, north, 0, is_last, core == 1),
    ]
    for start, inside, row, is_root, is_side in sides:
        for k in range(CHUNKS):
            part = at(slice(row + k * piece, row + (k + 1) * piece), every)
            root = jnp.logical_and(inside, is_root)
            holds = jnp.logical_and(inside, is_side)
            second = jnp.logical_and(holds, jnp.logical_not(is_root))
            receive(root, start + k, part)
            send(root, start + CHUNKS + k, part, part, t, far)
            receive(second, start + CHUNKS + k, part)
            send(holds, start + 2 * CHUNKS + k, part, part, t, near)
    receive(yes, 1, at(nears, mid))
    receive(yes, 7, at(nears, left))
    receive(yes, 8, at(nears, right))
    receive(yes, 6, at(nears_far, mid))
    receive(yes, 9, at(nears_far, left))
    receive(yes, 10, at(nears_far, right))
    convert(margin, margin + rows)
    for start, inside, row, is_root, is_side in sides:
        for k in range(CHUNKS):
            part = at(slice(row + k * piece, row + (k + 1) * piece), every)
            receive(jnp.logical_and(inside, jnp.logical_not(is_side)), start + 2 * CHUNKS + k, part)
    convert(0, margin)
    convert(margin + rows, tall)
    for cond, made in sent:
        @pl.when(cond)
        def _():
            made.wait_send()


def shared_sum(axis, devices, n_tile, n_pos, mine_ref, others, send_sems, recv_sems):
    copies = [
        pltpu.make_async_remote_copy(
            src_ref=mine_ref,
            dst_ref=others.at[k - 1],
            send_sem=send_sems.at[k - 1],
            recv_sem=recv_sems.at[k - 1],
            device_id=peer(axis, k, n_tile, n_pos),
            device_id_type=MESH_ID,
        )
        for k in range(1, devices)
    ]
    for made in copies:
        made.start()
    for made in copies:
        made.wait()
    return jnp.sum(others[...], axis=0) + mine_ref[...]


def fold(value):
    return jnp.sum(value.reshape(-1, 8, value.shape[-1]), axis=0)


def refine_kernel(
    batch, steps, n_tile, n_pos, off_ref, x_ref, probe_hbm, frames_ref, fwd_hbm, bwd_hbm, out_ref,
    pad_ref, probe_ref, fwd_ref, bwd_ref, planes, patch, slant, exits, halves, resid, inner, sums,
    send_sems, recv_sems, local_sems, pos_line, tile_line, pos_others, tile_others,
    pos_sends, pos_recvs, tile_sends, tile_recvs,
):
    step = pl.program_id(0)
    n = probe_ref.shape[1]
    tall, wide = pad_ref.shape[1], pad_ref.shape[2]
    lanes = 128
    blocks = n // lanes

    def convert(first, last):
        @pl.loop(first // 32, last // 32)
        def _(i):
            at = pl.ds(pl.multiple_of(i * 32, 32), 32)
            lower = pl.ds(pl.multiple_of(i * 32 + 8, 8), 32)
            for part in range(2):
                value = pad_ref[part, at, :].astype(jnp.float32)
                slope = 0.5 * (pltpu.roll(value, wide - 1, 1) - pltpu.roll(value, 1, 1))
                for k in range(wide // lanes):
                    cols = slice(k * lanes, (k + 1) * lanes)
                    planes[part, k, lower, :] = value[:, cols]
                    planes[2 + part, k, lower, :] = slope[:, cols]

    @pl.when(step == 0)
    def _():
        loads = [
            pltpu.make_async_copy(source, target, local_sems.at[k])
            for k, (source, target) in enumerate(((probe_hbm, probe_ref), (fwd_hbm, fwd_ref), (bwd_hbm, bwd_ref)))
        ]
        for load in loads:
            load.start()
        gather_halo(n_tile, n_pos, n // 2, x_ref, pad_ref, send_sems, recv_sems, local_sems.at[3], convert)
        for load in loads:
            load.wait()

    for b in range(batch):
        j = step * batch + b
        row, col = off_ref[0, j], off_ref[1, j]
        block, shift = col // lanes, col % lanes
        turn = (lanes - shift) % lanes
        for part in range(4):
            high = n + 8 if part < 2 else n
            first = row + 7 if part < 2 else row + 8
            target = patch.at[b, part] if part < 2 else slant.at[b, part - 2]
            keep = lax.broadcasted_iota(jnp.int32, (high, lanes), 1) < lanes - shift
            turned = [
                pltpu.roll(planes[part, block + k, pl.ds(first, high), :], turn, 1) for k in range(blocks + 1)
            ]
            for k in range(blocks):
                target[:, k * lanes : (k + 1) * lanes] = jnp.where(keep, turned[k], turned[k + 1])
        o_re, o_im = patch[b, 0, 1 : n + 1, :], patch[b, 1, 1 : n + 1, :]
        p_re, p_im = probe_ref[0], probe_ref[1]
        exits[b, :n, :] = (p_re * o_re - p_im * o_im).astype(jnp.bfloat16)
        exits[b, n:, :] = (p_re * o_im + p_im * o_re).astype(jnp.bfloat16)
    for b in range(batch):
        half = jnp.dot(fwd_ref[...], exits[b], preferred_element_type=jnp.float32)
        halves[b * n : (b + 1) * n, :n] = half[:n].astype(jnp.bfloat16)
        halves[b * n : (b + 1) * n, n:] = half[n:].astype(jnp.bfloat16)
    losses = []
    for b in range(batch):
        wave = jnp.dot(halves[b * n : (b + 1) * n, :], bwd_ref[...], preferred_element_type=jnp.float32)
        f_re, f_im = wave[:, :n], wave[:, n:]
        square = f_re * f_re + f_im * f_im
        keep_part = 1.0 - frames_ref[b].astype(jnp.float32) * lax.rsqrt(jnp.maximum(square, 0.0625))
        losses.append(fold(square * (keep_part * keep_part)))
        resid[b, :n, :] = (f_re * keep_part).astype(jnp.bfloat16)
        resid[b, n:, :] = (f_im * keep_part).astype(jnp.bfloat16)
    for b in range(batch):
        back = jnp.dot(bwd_ref[...], resid[b], preferred_element_type=jnp.float32)
        inner[b * n : (b + 1) * n, :n] = back[:n].astype(jnp.bfloat16)
        inner[b * n : (b + 1) * n, n:] = back[n:].astype(jnp.bfloat16)
    for b in range(batch):
        j = step * batch + b
        wave = jnp.dot(inner[b * n : (b + 1) * n, :], fwd_ref[...], preferred_element_type=jnp.float32)
        g_re, g_im = wave[:, :n], wave[:, n:]
        p_re, p_im = probe_ref[0], probe_ref[1]
        q_re = g_re * p_re + g_im * p_im
        q_im = g_re * p_im - g_im * p_re
        d_re = patch[b, 0, 2 : n + 2, :] - patch[b, 0, 0:n, :]
        d_im = patch[b, 1, 2 : n + 2, :] - patch[b, 1, 0:n, :]
        by_row = fold(q_re * d_re - q_im * d_im) * 0.5
        by_col = fold(q_re * slant[b, 0] - q_im * slant[b, 1])
        for which, value in enumerate((by_row, by_col, losses[b] * (1.0 / (n * n)))):
            line = jnp.sum(value, axis=0, keepdims=True)
            short = line[:, :lanes]
            for k in range(1, blocks):
                short = short + line[:, k * lanes : (k + 1) * lanes]
            sums[which, pl.ds(j, 1), :] = short

    @pl.when(step == steps - 1)
    def _():
        count = sums.shape[1]
        diagonal = lax.broadcasted_iota(jnp.int32, (count, lanes), 0) == lax.broadcasted_iota(jnp.int32, (count, lanes), 1)
        lines = []
        for which in range(3):
            full = jnp.sum(sums[which], axis=1, keepdims=True)
            lines.append(jnp.sum(jnp.where(diagonal, full, 0.0), axis=0, keepdims=True))
        squares = jnp.sum(lines[0] * lines[0] + lines[1] * lines[1], axis=1, keepdims=True)
        pos_line[...] = jnp.broadcast_to(squares, (1, lanes))
        tile_line[...] = shared_sum("pos", n_pos, n_tile, n_pos, pos_line, pos_others, pos_sends, pos_recvs)
        lines.append(shared_sum("tile", n_tile, n_tile, n_pos, tile_line, tile_others, tile_sends, tile_recvs))
        out_ref[...] = jnp.concatenate(lines + [jnp.zeros((4, lanes), jnp.float32)], axis=0)


def refine(quarter, probe, frames, offsets, n_tile, n_pos):
    count, n, _ = frames.shape
    _, height, width = quarter.shape
    if count % BATCH or count > 128 or n % 128 or n_pos != 4 or height < n // 2:
        raise ValueError("unsupported sizes")
    forward, backward = dft_tables(n)
    tall, wide = height * n_pos + n, width + n
    steps = count // BATCH
    sems = 11 + 6 * CHUNKS
    vmem, dma = pltpu.VMEM, pltpu.SemaphoreType.DMA
    whole = lambda shape: pl.BlockSpec(shape, lambda i: (0,) * len(shape))
    anywhere = pl.BlockSpec(memory_space=pl.ANY)
    return pl.pallas_call(
        functools.partial(refine_kernel, BATCH, steps, n_tile, n_pos),
        grid=(steps,),
        out_shape=jax.ShapeDtypeStruct((8, 128), jnp.float32),
        in_specs=[
            pl.BlockSpec(memory_space=pltpu.SMEM),
            whole(quarter.shape),
            anywhere,
            pl.BlockSpec((BATCH, n, n), lambda i: (i, 0, 0)),
            anywhere,
            anywhere,
        ],
        out_specs=whole((8, 128)),
        scratch_shapes=[
            vmem((2, tall, wide), jnp.bfloat16),
            vmem(probe.shape, jnp.float32),
            vmem(forward.shape, jnp.bfloat16),
            vmem(backward.shape, jnp.bfloat16),
            vmem((4, wide // 128, tall + 16, 128), jnp.float32),
            vmem((BATCH, 2, n + 8, n), jnp.float32),
            vmem((BATCH, 2, n, n), jnp.float32),
            vmem((BATCH, 2 * n, n), jnp.bfloat16),
            vmem((BATCH * n, 2 * n), jnp.bfloat16),
            vmem((BATCH, 2 * n, n), jnp.bfloat16),
            vmem((BATCH * n, 2 * n), jnp.bfloat16),
            vmem((3, count, 128), jnp.float32),
            dma((sems,)),
            dma((sems,)),
            dma((4,)),
            vmem((1, 128), jnp.float32),
            vmem((1, 128), jnp.float32),
            vmem((n_pos - 1, 1, 128), jnp.float32),
            vmem((n_tile - 1, 1, 128), jnp.float32),
            dma((n_pos - 1,)),
            dma((n_pos - 1,)),
            dma((n_tile - 1,)),
            dma((n_tile - 1,)),
        ],
        compiler_params=pltpu.CompilerParams(
            vmem_limit_bytes=56 * 1024 * 1024, collective_id=0, has_side_effects=True
        ),
    )(offsets, quarter, probe, frames, forward, backward)


def scale_kernel(positions, lines_ref, shifts_ref, losses_ref):
    count = shifts_ref.shape[1]
    scale = jnp.sqrt(lines_ref[3:4, :] * (1.0 / positions) + 1e-06)
    shifts_ref[...] = (-lines_ref[0:2, :] / scale)[:, :count]
    losses_ref[...] = lines_ref[2:3, :count]


def normalise(lines, count, positions):
    block = pl.BlockSpec(memory_space=pltpu.VMEM)
    return pl.pallas_call(
        functools.partial(scale_kernel, positions),
        out_shape=(jax.ShapeDtypeStruct((2, count), jnp.float32), jax.ShapeDtypeStruct((1, count), jnp.float32)),
        in_specs=[block],
        out_specs=(block, block),
    )(lines)


def solution(mesh):
    n_tile, n_pos = mesh.shape["tile"], mesh.shape["pos"]

    def local(object_tiles, probe, frames, offsets):
        count = frames.shape[0]
        lines = refine(object_tiles[0], probe, frames, offsets, n_tile, n_pos)
        shifts, losses = normalise(lines, count, count * n_tile * n_pos)
        return shifts, losses[0]

    in_specs = (
        P("tile", None, "pos", None),
        P(),
        P(("tile", "pos"), None, None),
        P(None, ("tile", "pos")),
    )
    out_specs = (P(None, ("tile", "pos")), P(("tile", "pos")))
    return jax.shard_map(local, mesh=mesh, in_specs=in_specs, out_specs=out_specs, check_vma=False)
```

```python
import functools
import math

import jax
import jax.numpy as jnp
import numpy as np
from jax import lax
from jax.experimental import pallas as pl
from jax.experimental.pallas import tpu as pltpu
from jax.sharding import PartitionSpec as P

GC = 4
CHUNKS = 4
BATCH = 4
MESH_ID = pl.DeviceIdType.MESH


def dft_tables(length_n):
    indices = np.arange(length_n)
    products_mod = indices[:, None] * indices[None, :] % length_n
    angles = products_mod.astype(np.float32) * np.float32(2.0 * math.pi / length_n)
    factor = np.float32(1.0 / math.sqrt(length_n))
    cosine, sine = np.cos(angles) * factor, np.sin(angles) * factor
    forward = np.block([[cosine, sine], [-sine, cosine]])
    return jnp.asarray(forward, jnp.bfloat16), jnp.asarray(forward.T, jnp.bfloat16)


def peer(axis, k, n_tile, n_pos):
    t, p = lax.axis_index("tile"), lax.axis_index("pos")
    if axis == "pos":
        return (t, lax.rem(p + k, n_pos))
    return (lax.rem(t + k, n_tile), p)


def gather_halo(n_tile, n_pos, margin, x_ref, pad_ref, send_sems, recv_sems, local_sem, convert):
    t, p = lax.axis_index("tile"), lax.axis_index("pos")
    _, quarter, width = x_ref.shape
    rows = pad_ref.shape[1] - 2 * margin
    last = rows // quarter - 1
    c, r = t % GC, t // GC
    core, half = p % 2, p // 2
    near, far = p + 1 - 2 * core, p + 2 - 4 * half
    west, east = c > 0, c < GC - 1
    north, south = r > 0, r < n_tile // GC - 1
    yes = p >= 0
    is_first, is_last = p == 0, p == last
    tall, wide = rows + 2 * margin, width + 2 * margin

    def zero(cond, rows_at, cols_at):
        @pl.when(cond)
        def _():
            part = pad_ref.at[:, rows_at, cols_at]
            part[...] = jnp.zeros(part.shape, part.dtype)

    zero(jnp.logical_not(west), slice(0, tall), slice(0, margin))
    zero(jnp.logical_not(east), slice(0, tall), slice(margin + width, wide))
    zero(jnp.logical_not(north), slice(0, margin), slice(0, wide))
    zero(jnp.logical_not(south), slice(margin + rows, tall), slice(0, wide))

    barrier = pltpu.get_barrier_semaphore()
    for axis, devices in (("pos", n_pos), ("tile", n_tile)):
        for k in range(1, devices):
            pl.semaphore_signal(barrier, inc=1, device_id=peer(axis, k, n_tile, n_pos), device_id_type=MESH_ID)
    pl.semaphore_wait(barrier, n_pos + n_tile - 2)

    mine = pl.ds(pl.multiple_of(margin + p * quarter, quarter), quarter)
    its = pl.ds(pl.multiple_of(margin + far * quarter, quarter), quarter)
    nears = pl.ds(pl.multiple_of(margin + near * quarter, quarter), quarter)
    near_far = near + 2 - 4 * half
    nears_far = pl.ds(pl.multiple_of(margin + near_far * quarter, quarter), quarter)
    mid = slice(margin, margin + width)
    left, right = slice(0, margin), slice(margin + width, wide)
    every = slice(0, wide)
    sent = []

    def copy(index, src, dst, to_t, to_p):
        return pltpu.make_async_remote_copy(
            src_ref=src,
            dst_ref=dst,
            send_sem=send_sems.at[index],
            recv_sem=recv_sems.at[index],
            device_id=(to_t, to_p),
            device_id_type=MESH_ID,
        )

    def send(cond, index, src, dst, to_t, to_p):
        made = copy(index, src, dst, to_t, to_p)
        sent.append((cond, made))

        @pl.when(cond)
        def _():
            made.start()

    def receive(cond, index, dst):
        @pl.when(cond)
        def _():
            copy(index, dst, dst, t, near).wait_recv()

    def at(rows_at, cols_at):
        return pad_ref.at[:, rows_at, cols_at]

    own = pltpu.make_async_copy(x_ref, at(mine, mid), local_sem)
    own.start()
    send(east, 2, x_ref.at[:, :, width - margin : width], at(mine, left), t + 1, p)
    send(west, 3, x_ref.at[:, :, 0:margin], at(mine, right), t - 1, p)
    send(yes, 0, x_ref, at(mine, mid), t, far)
    send(yes, 1, x_ref, at(mine, mid), t, near)
    own.wait()
    receive(west, 2, at(mine, left))
    receive(east, 3, at(mine, right))
    piece = margin // CHUNKS
    base = 11
    for k in range(CHUNKS):
        up, down = slice(margin + rows + k * piece, margin + rows + (k + 1) * piece), slice(k * piece, (k + 1) * piece)
        top = slice(margin + k * piece, margin + (k + 1) * piece)
        bottom = slice(rows + k * piece, rows + (k + 1) * piece)
        send(jnp.logical_and(is_first, north), base + k, at(top, every), at(up, every), t - GC, p)
        send(jnp.logical_and(is_last, south), base + 3 * CHUNKS + k, at(bottom, every), at(down, every), t + GC, p)
    send(yes, 4, at(mine, left), at(mine, left), t, far)
    send(yes, 5, at(mine, right), at(mine, right), t, far)
    send(yes, 7, at(mine, left), at(mine, left), t, near)
    send(yes, 8, at(mine, right), at(mine, right), t, near)
    receive(yes, 0, at(its, mid))
    send(yes, 6, at(its, mid), at(its, mid), t, near)
    receive(yes, 4, at(its, left))
    send(yes, 9, at(its, left), at(its, left), t, near)
    receive(yes, 5, at(its, right))
    send(yes, 10, at(its, right), at(its, right), t, near)
    sides = [
        (base, south, margin + rows, is_first, core == 0),
        (base + 3 * CHUNKS, north, 0, is_last, core == 1),
    ]
    for start, inside, row, is_root, is_side in sides:
        for k in range(CHUNKS):
            part = at(slice(row + k * piece, row + (k + 1) * piece), every)
            root = jnp.logical_and(inside, is_root)
            holds = jnp.logical_and(inside, is_side)
            second = jnp.logical_and(holds, jnp.logical_not(is_root))
            receive(root, start + k, part)
            send(root, start + CHUNKS + k, part, part, t, far)
            receive(second, start + CHUNKS + k, part)
            send(holds, start + 2 * CHUNKS + k, part, part, t, near)
    receive(yes, 1, at(nears, mid))
    receive(yes, 7, at(nears, left))
    receive(yes, 8, at(nears, right))
    receive(yes, 6, at(nears_far, mid))
    receive(yes, 9, at(nears_far, left))
    receive(yes, 10, at(nears_far, right))
    convert(margin, margin + rows)
    for start, inside, row, is_root, is_side in sides:
        for k in range(CHUNKS):
            part = at(slice(row + k * piece, row + (k + 1) * piece), every)
            receive(jnp.logical_and(inside, jnp.logical_not(is_side)), start + 2 * CHUNKS + k, part)
    convert(0, margin)
    convert(margin + rows, tall)
    for cond, made in sent:
        @pl.when(cond)
        def _():
            made.wait_send()


def shared_sum(axis, devices, n_tile, n_pos, mine_ref, others, send_sems, recv_sems):
    copies = [
        pltpu.make_async_remote_copy(
            src_ref=mine_ref,
            dst_ref=others.at[k - 1],
            send_sem=send_sems.at[k - 1],
            recv_sem=recv_sems.at[k - 1],
            device_id=peer(axis, k, n_tile, n_pos),
            device_id_type=MESH_ID,
        )
        for k in range(1, devices)
    ]
    for made in copies:
        made.start()
    for made in copies:
        made.wait()
    return jnp.sum(others[...], axis=0) + mine_ref[...]


def fold(value):
    return jnp.sum(value.reshape(-1, 8, value.shape[-1]), axis=0)


def refine_kernel(
    batch, steps, n_tile, n_pos, off_ref, x_ref, probe_hbm, frames_ref, fwd_hbm, bwd_hbm, out_ref,
    pad_ref, probe_ref, fwd_ref, bwd_ref, planes, patch, slant, exits, halves, resid, inner, sums,
    send_sems, recv_sems, local_sems, pos_line, tile_line, pos_others, tile_others,
    pos_sends, pos_recvs, tile_sends, tile_recvs,
):
    step = pl.program_id(0)
    n = probe_ref.shape[1]
    tall, wide = pad_ref.shape[1], pad_ref.shape[2]
    lanes = 128
    blocks = n // lanes

    def convert(first, last):
        @pl.loop(first // 32, last // 32)
        def _(i):
            at = pl.ds(pl.multiple_of(i * 32, 32), 32)
            lower = pl.ds(pl.multiple_of(i * 32 + 8, 8), 32)
            for part in range(2):
                value = pad_ref[part, at, :].astype(jnp.float32)
                slope = 0.5 * (pltpu.roll(value, wide - 1, 1) - pltpu.roll(value, 1, 1))
                for k in range(wide // lanes):
                    cols = slice(k * lanes, (k + 1) * lanes)
                    planes[part, k, lower, :] = value[:, cols]
                    planes[2 + part, k, lower, :] = slope[:, cols]

    @pl.when(step == 0)
    def _():
        loads = [
            pltpu.make_async_copy(source, target, local_sems.at[k])
            for k, (source, target) in enumerate(((probe_hbm, probe_ref), (fwd_hbm, fwd_ref), (bwd_hbm, bwd_ref)))
        ]
        for load in loads:
            load.start()
        gather_halo(n_tile, n_pos, n // 2, x_ref, pad_ref, send_sems, recv_sems, local_sems.at[3], convert)
        for load in loads:
            load.wait()

    for b in range(batch):
        j = step * batch + b
        row, col = off_ref[0, j], off_ref[1, j]
        block, shift = col // lanes, col % lanes
        turn = (lanes - shift) % lanes
        for part in range(4):
            high = n + 8 if part < 2 else n
            first = row + 7 if part < 2 else row + 8
            target = patch.at[b, part] if part < 2 else slant.at[b, part - 2]
            keep = lax.broadcasted_iota(jnp.int32, (high, lanes), 1) < lanes - shift
            turned = [
                pltpu.roll(planes[part, block + k, pl.ds(first, high), :], turn, 1) for k in range(blocks + 1)
            ]
            for k in range(blocks):
                target[:, k * lanes : (k + 1) * lanes] = jnp.where(keep, turned[k], turned[k + 1])
        o_re, o_im = patch[b, 0, 1 : n + 1, :], patch[b, 1, 1 : n + 1, :]
        p_re, p_im = probe_ref[0], probe_ref[1]
        exits[b, :n, :] = (p_re * o_re - p_im * o_im).astype(jnp.bfloat16)
        exits[b, n:, :] = (p_re * o_im + p_im * o_re).astype(jnp.bfloat16)
    for b in range(batch):
        half = jnp.dot(fwd_ref[...], exits[b], preferred_element_type=jnp.float32)
        halves[b * n : (b + 1) * n, :n] = half[:n].astype(jnp.bfloat16)
        halves[b * n : (b + 1) * n, n:] = half[n:].astype(jnp.bfloat16)
    losses = []
    for b in range(batch):
        wave = jnp.dot(halves[b * n : (b + 1) * n, :], bwd_ref[...], preferred_element_type=jnp.float32)
        f_re, f_im = wave[:, :n], wave[:, n:]
        square = f_re * f_re + f_im * f_im
        keep_part = 1.0 - frames_ref[b].astype(jnp.float32) * lax.rsqrt(jnp.maximum(square, 0.0625))
        losses.append(fold(square * (keep_part * keep_part)))
        resid[b, :n, :] = (f_re * keep_part).astype(jnp.bfloat16)
        resid[b, n:, :] = (f_im * keep_part).astype(jnp.bfloat16)
    for b in range(batch):
        back = jnp.dot(bwd_ref[...], resid[b], preferred_element_type=jnp.float32)
        inner[b * n : (b + 1) * n, :n] = back[:n].astype(jnp.bfloat16)
        inner[b * n : (b + 1) * n, n:] = back[n:].astype(jnp.bfloat16)
    for b in range(batch):
        j = step * batch + b
        wave = jnp.dot(inner[b * n : (b + 1) * n, :], fwd_ref[...], preferred_element_type=jnp.float32)
        g_re, g_im = wave[:, :n], wave[:, n:]
        p_re, p_im = probe_ref[0], probe_ref[1]
        q_re = g_re * p_re + g_im * p_im
        q_im = g_re * p_im - g_im * p_re
        d_re = patch[b, 0, 2 : n + 2, :] - patch[b, 0, 0:n, :]
        d_im = patch[b, 1, 2 : n + 2, :] - patch[b, 1, 0:n, :]
        by_row = fold(q_re * d_re - q_im * d_im) * 0.5
        by_col = fold(q_re * slant[b, 0] - q_im * slant[b, 1])
        for which, value in enumerate((by_row, by_col, losses[b] * (1.0 / (n * n)))):
            line = jnp.sum(value, axis=0, keepdims=True)
            short = line[:, :lanes]
            for k in range(1, blocks):
                short = short + line[:, k * lanes : (k + 1) * lanes]
            sums[which, pl.ds(j, 1), :] = short

    @pl.when(step == steps - 1)
    def _():
        count = sums.shape[1]
        diagonal = lax.broadcasted_iota(jnp.int32, (count, lanes), 0) == lax.broadcasted_iota(jnp.int32, (count, lanes), 1)
        lines = []
        for which in range(3):
            full = jnp.sum(sums[which], axis=1, keepdims=True)
            lines.append(jnp.sum(jnp.where(diagonal, full, 0.0), axis=0, keepdims=True))
        squares = jnp.sum(lines[0] * lines[0] + lines[1] * lines[1], axis=1, keepdims=True)
        pos_line[...] = jnp.broadcast_to(squares, (1, lanes))
        tile_line[...] = shared_sum("pos", n_pos, n_tile, n_pos, pos_line, pos_others, pos_sends, pos_recvs)
        lines.append(shared_sum("tile", n_tile, n_tile, n_pos, tile_line, tile_others, tile_sends, tile_recvs))
        out_ref[...] = jnp.concatenate(lines + [jnp.zeros((4, lanes), jnp.float32)], axis=0)


def refine(quarter, probe, frames, offsets, n_tile, n_pos):
    count, n, _ = frames.shape
    _, height, width = quarter.shape
    if count % BATCH or count > 128 or n % 128 or n_pos != 4 or height < n // 2:
        raise ValueError("unsupported sizes")
    forward, backward = dft_tables(n)
    tall, wide = height * n_pos + n, width + n
    steps = count // BATCH
    sems = 11 + 6 * CHUNKS
    vmem, dma = pltpu.VMEM, pltpu.SemaphoreType.DMA
    whole = lambda shape: pl.BlockSpec(shape, lambda i: (0,) * len(shape))
    anywhere = pl.BlockSpec(memory_space=pl.ANY)
    return pl.pallas_call(
        functools.partial(refine_kernel, BATCH, steps, n_tile, n_pos),
        grid=(steps,),
        out_shape=jax.ShapeDtypeStruct((8, 128), jnp.float32),
        in_specs=[
            pl.BlockSpec(memory_space=pltpu.SMEM),
            whole(quarter.shape),
            anywhere,
            pl.BlockSpec((BATCH, n, n), lambda i: (i, 0, 0)),
            anywhere,
            anywhere,
        ],
        out_specs=whole((8, 128)),
        scratch_shapes=[
            vmem((2, tall, wide), jnp.bfloat16),
            vmem(probe.shape, jnp.float32),
            vmem(forward.shape, jnp.bfloat16),
            vmem(backward.shape, jnp.bfloat16),
            vmem((4, wide // 128, tall + 16, 128), jnp.float32),
            vmem((BATCH, 2, n + 8, n), jnp.float32),
            vmem((BATCH, 2, n, n), jnp.float32),
            vmem((BATCH, 2 * n, n), jnp.bfloat16),
            vmem((BATCH * n, 2 * n), jnp.bfloat16),
            vmem((BATCH, 2 * n, n), jnp.bfloat16),
            vmem((BATCH * n, 2 * n), jnp.bfloat16),
            vmem((3, count, 128), jnp.float32),
            dma((sems,)),
            dma((sems,)),
            dma((4,)),
            vmem((1, 128), jnp.float32),
            vmem((1, 128), jnp.float32),
            vmem((n_pos - 1, 1, 128), jnp.float32),
            vmem((n_tile - 1, 1, 128), jnp.float32),
            dma((n_pos - 1,)),
            dma((n_pos - 1,)),
            dma((n_tile - 1,)),
            dma((n_tile - 1,)),
        ],
        compiler_params=pltpu.CompilerParams(
            vmem_limit_bytes=56 * 1024 * 1024, collective_id=0, has_side_effects=True
        ),
    )(offsets, quarter, probe, frames, forward, backward)


def scale_kernel(positions, lines_ref, shifts_ref, losses_ref):
    count = shifts_ref.shape[1]
    scale = jnp.sqrt(lines_ref[3:4, :] * (1.0 / positions) + 1e-06)
    shifts_ref[...] = (-lines_ref[0:2, :] / scale)[:, :count]
    losses_ref[...] = lines_ref[2:3, :count]


def normalise(lines, count, positions):
    block = pl.BlockSpec(memory_space=pltpu.VMEM)
    return pl.pallas_call(
        functools.partial(scale_kernel, positions),
        out_shape=(jax.ShapeDtypeStruct((2, count), jnp.float32), jax.ShapeDtypeStruct((1, count), jnp.float32)),
        in_specs=[block],
        out_specs=(block, block),
    )(lines)


def solution(mesh):
    n_tile, n_pos = mesh.shape["tile"], mesh.shape["pos"]

    def local(object_tiles, probe, frames, offsets):
        count = frames.shape[0]
        lines = refine(object_tiles[0], probe, frames, offsets, n_tile, n_pos)
        shifts, losses = normalise(lines, count, count * n_tile * n_pos)
        return shifts, losses[0]

    in_specs = (
        P("tile", None, "pos", None),
        P(),
        P(("tile", "pos"), None, None),
        P(None, ("tile", "pos")),
    )
    out_specs = (P(None, ("tile", "pos")), P(("tile", "pos")))
    return jax.shard_map(local, mesh=mesh, in_specs=in_specs, out_specs=out_specs, check_vma=False)
```
